32 devices in a mesh: dp: 4 (over z), row: 2 (over x), col: 4 (over y, core).
Axes of the slice: x: 2, y: 2, z: 4, core: 2. Of those that a mesh axis runs over, the one named last changes fastest.
Arguments:
- inputs: bfloat16 [4096, 1536], P(('dp', 'row'), 'col'), may hold values from -12.5 to 12.5
- gain_attn: bfloat16 [1536], P(('col', 'dp')), may hold values from 0.25 to 1.75
- w_query: bfloat16 [1536, 1536], P(('col', 'dp'), 'row'), may hold values from -0.15625 to 0.15625
- b_query: bfloat16 [1536], P(('row', 'dp')), may hold values from -3 to 3
- key_weight: bfloat16 [1536, 256], P(('col', 'dp'), 'row'), may hold values from -0.15625 to 0.15625
- key_bias: bfloat16 [256], P(('row', 'dp')), may hold values from -3 to 3
- value_weight: bfloat16 [1536, 256], P(('col', 'dp'), 'row'), may hold values from -0.15625 to 0.15625
- value_bias: bfloat16 [256], P(('row', 'dp')), may hold values from -3 to 3
- w_output: bfloat16 [1536, 1536], P(('row', 'dp'), 'col'), may hold values from -1.25 to 1.25
- gain_mlp: bfloat16 [1536], P(('col', 'dp')), may hold values from 0.25 to 1.75
- w_gate: bfloat16 [1536, 8960], P(('col', 'dp'), 'row'), may hold values from -0.15625 to 0.15625
- w_up: bfloat16 [1536, 8960], P(('col', 'dp'), 'row'), may hold values from -0.15625 to 0.15625
- w_down: bfloat16 [8960, 1536], P(('row', 'dp'), 'col'), may hold values from -0.0625 to 0.0625
- cotangent: bfloat16 [4096, 1536], P(('dp', 'row'), 'col'), may hold values from -6 to 6
Outputs:
- outputs: bfloat16 [4096, 1536], P(('dp', 'row'), 'col')
- grad_inputs: bfloat16 [4096, 1536], P(('dp', 'row'), 'col')
- grad_gain_attn: float32 [1536], P(('col', 'dp'))
- grad_w_query: float32 [1536, 1536], P(('col', 'dp'), 'row')
- grad_b_query: float32 [1536], P(('row', 'dp'))
- grad_w_key: float32 [1536, 256], P(('col', 'dp'), 'row')
- grad_b_key: float32 [256], P(('row', 'dp'))
- grad_w_value: float32 [1536, 256], P(('col', 'dp'), 'row')
- grad_b_value: float32 [256], P(('row', 'dp'))
- grad_w_output: float32 [1536, 1536], P(('row', 'dp'), 'col')
- grad_gain_mlp: float32 [1536], P(('col', 'dp'))
- grad_w_gate: float32 [1536, 8960], P(('col', 'dp'), 'row')
- grad_w_up: float32 [1536, 8960], P(('col', 'dp'), 'row')
- grad_w_down: float32 [8960, 1536], P(('row', 'dp'), 'col')
The draws below stay inside these ranges and needn't reach their ends.
All inputs are finite; a program needn't handle non-finite values.
Results may differ from the reference program's by a relative error of at most 0.025.
Values may be sent and summed in bfloat16 or wider, within the bound.
A program may use at most 256 MiB of HBM per device.

```python
import jax
import jax.numpy as jnp
from jax import lax

MODEL_WIDTH = 1536
QUERY_HEADS = 12
KEY_VALUE_HEADS = 2
HEAD_SIZE = 128
FF = 8960
SEQ = 1024
TOKENS = 4096
N_DP = 4


def draw_inputs(key, part):
    key_values = jax.random.fold_in(key, 11)
    key_rough = jax.random.fold_in(key, 12)
    place = jnp.arange(MODEL_WIDTH, dtype=jnp.float32) / (MODEL_WIDTH - 1)
    rough = jax.random.uniform(key_rough, (MODEL_WIDTH,), jnp.float32, 0.7, 1.4)
    profile = 10.0 ** place / 4.6
    values = jax.random.truncated_normal(key_values, -4.0, 4.0, (TOKENS, MODEL_WIDTH), jnp.float32)
    return (values * (profile * rough)[None, :]).astype(jnp.bfloat16)


def shard_levels(stream_key, dims, pieces, low, high):
    def one(dim, shards_of):
        steps = jax.random.uniform(jax.random.fold_in(jax.random.fold_in(stream_key, 6), dim), (shards_of,), jnp.float32, low / len(pieces), high / len(pieces))
        return jnp.repeat(jnp.exp(steps), dims[dim] // shards_of).reshape((-1,) + (1,) * (len(dims) - dim - 1))

    loudness = one(*pieces[0])
    for cut in pieces[1:]:
        loudness = loudness * one(*cut)
    return loudness


def gaussian(key, dims, width, reach, cuts=(), held_as=jnp.bfloat16):
    entries = width * jax.random.normal(key, dims, jnp.float32)
    if cuts:
        entries = entries * shard_levels(key, dims, cuts, -0.22, 0.18)
    return jnp.clip(entries, -reach, reach).astype(held_as)


def setup_inputs(seed: int = 0) -> dict:
    key_of = jax.random.split(jax.random.key(seed), 15)
    return {
        "inputs": draw_inputs(jax.random.fold_in(key_of[14], 71), 0),
        "gain_attn": jnp.clip(1.0 + 0.15 * jax.random.normal(key_of[1], (MODEL_WIDTH,), jnp.float32), 0.25, 1.75).astype(jnp.bfloat16),
        "w_query": gaussian(key_of[2], (MODEL_WIDTH, QUERY_HEADS * HEAD_SIZE), MODEL_WIDTH ** -0.5, 0.15625, ((0, 16), (1, 2))),
        "b_query": gaussian(key_of[3], (QUERY_HEADS * HEAD_SIZE,), 0.5, 3.0, ((0, 8),)),
        "key_weight": gaussian(key_of[4], (MODEL_WIDTH, KEY_VALUE_HEADS * HEAD_SIZE), MODEL_WIDTH ** -0.5, 0.15625, ((0, 16), (1, 2))),
        "key_bias": gaussian(key_of[5], (KEY_VALUE_HEADS * HEAD_SIZE,), 0.5, 3.0, ((0, 8),)),
        "value_weight": gaussian(key_of[6], (MODEL_WIDTH, KEY_VALUE_HEADS * HEAD_SIZE), MODEL_WIDTH ** -0.5, 0.15625, ((0, 16), (1, 2))),
        "value_bias": gaussian(key_of[7], (KEY_VALUE_HEADS * HEAD_SIZE,), 0.5, 3.0, ((0, 8),)),
        "w_output": gaussian(key_of[8], (QUERY_HEADS * HEAD_SIZE, MODEL_WIDTH), (QUERY_HEADS * HEAD_SIZE // 64) ** -0.5, 1.25, ((0, 8), (1, 4))),
        "gain_mlp": jnp.clip(1.0 + 0.15 * jax.random.normal(key_of[9], (MODEL_WIDTH,), jnp.float32), 0.25, 1.75).astype(jnp.bfloat16),
        "w_gate": gaussian(key_of[10], (MODEL_WIDTH, FF), MODEL_WIDTH ** -0.5, 0.15625, ((0, 16), (1, 2))),
        "w_up": gaussian(key_of[11], (MODEL_WIDTH, FF), MODEL_WIDTH ** -0.5, 0.15625, ((0, 16), (1, 2))),
        "w_down": gaussian(key_of[12], (FF, MODEL_WIDTH), FF ** -0.5, 0.0625, ((0, 8), (1, 4))),
        "cotangent": gaussian(key_of[13], (TOKENS, MODEL_WIDTH), 1.0, 6.0, ((0, 8), (1, 4))),
    }


@jax.custom_vjp
def low(v):
    return lax.optimization_barrier(v.astype(jnp.bfloat16)).astype(jnp.float32)

@jax.custom_vjp
def low_back(v):
    return v

def low_keep(v):
    return (low(v), None)

def low_pass(kept, grad):
    return (grad,)

def back_keep(v):
    return (v, None)

def back_low(kept, grad):
    return (low(grad),)
low.defvjp(low_keep, low_pass)
low_back.defvjp(back_keep, back_low)
epsilon = 1e-06
rope_base = 1000000.0
highest = lax.Precision.HIGHEST

def matmul(left, right):
    return jnp.dot(left, right, precision=highest)

def rms_norm(value_rows, gain):
    return value_rows * lax.rsqrt(lax.optimization_barrier(jnp.mean(value_rows * value_rows, axis=-1, keepdims=True)) + epsilon) * gain

def rope_turn(value_rows, positions, direction):
    row_count = value_rows.shape[0]
    heads = value_rows.shape[1] // HEAD_SIZE
    half = HEAD_SIZE // 2
    freqs = rope_base ** (-(jnp.arange(half, dtype=jnp.float32) * 2.0 / HEAD_SIZE))
    angles = positions.astype(jnp.float32)[:, None] * freqs[None, :]
    cosine = jnp.cos(angles)[:, None, :]
    sine = direction * jnp.sin(angles)[:, None, :]
    shaped = value_rows.reshape(row_count, heads, HEAD_SIZE)
    first = shaped[..., :half]
    second = shaped[..., half:]
    turned = jnp.concatenate([first * cosine - second * sine, second * cosine + first * sine], -1)
    return turned.reshape(row_count, heads * HEAD_SIZE)

def layer(inputs, gain_attn, w_query, b_query, key_weight, key_bias, value_weight, value_bias, w_output, gain_mlp, w_gate, w_up, w_down):
    sequence_length = inputs.shape[0]
    positions = jnp.arange(sequence_length, dtype=jnp.int32)
    normed1 = low(rms_norm(inputs, gain_attn))
    q_pre = low_back(matmul(normed1, w_query) + b_query)
    k_pre = low_back(matmul(normed1, key_weight) + key_bias)
    value_rows = low(low_back(matmul(normed1, value_weight) + value_bias))
    query_rows = low(rope_turn(q_pre, positions, 1.0))
    rotated_keys = low(rope_turn(k_pre, positions, 1.0))
    heads_per_group = QUERY_HEADS // KEY_VALUE_HEADS
    rows_per_block = min(512, sequence_length)
    count_of_blocks = sequence_length // rows_per_block
    blocks_of_queries = query_rows.reshape(count_of_blocks, rows_per_block, KEY_VALUE_HEADS, heads_per_group, HEAD_SIZE)
    keys_triple_shape = rotated_keys.reshape(sequence_length, KEY_VALUE_HEADS, HEAD_SIZE)
    values_triple_shape = value_rows.reshape(sequence_length, KEY_VALUE_HEADS, HEAD_SIZE)
    starts = jnp.arange(count_of_blocks, dtype=jnp.int32) * rows_per_block

    def one_block(first_row, query_part, key_part, value_part):
        raw = jnp.einsum('ikgd,jkd->kgij', query_part, key_part, precision=highest)
        scores = low_back(raw * HEAD_SIZE ** (-0.5))
        admitted = jnp.arange(sequence_length, dtype=jnp.int32)[None, :] <= (first_row + jnp.arange(rows_per_block, dtype=jnp.int32))[:, None]
        scores = jnp.where(admitted, scores, -1e+30)
        top_score = lax.optimization_barrier(jnp.max(scores, axis=-1, keepdims=True))
        expo = jnp.exp(scores - top_score)
        probs = low(expo / lax.optimization_barrier(jnp.sum(expo, axis=-1, keepdims=True)))
        return jnp.einsum('kgij,jkd->ikgd', probs, value_part, precision=highest)
    checked = jax.checkpoint(one_block)
    blocks_out = lax.map(lambda entry_pair: checked(entry_pair[0], entry_pair[1], keys_triple_shape, values_triple_shape), (starts, blocks_of_queries))
    attended = low(low_back(blocks_out.reshape(sequence_length, QUERY_HEADS * HEAD_SIZE)))
    middle = inputs + low_back(matmul(attended, w_output))
    normed2 = low(rms_norm(middle, gain_mlp))
    gate_pre = low_back(matmul(normed2, w_gate))
    up_pre = low_back(matmul(normed2, w_up))
    hidden = low(jax.nn.silu(gate_pre) * up_pre)
    return middle + low_back(matmul(hidden, w_down))

def reference(inputs, gain_attn, w_query, b_query, key_weight, key_bias, value_weight, value_bias, w_output, gain_mlp, w_gate, w_up, w_down, cotangent):
    weights = tuple((item_w.astype(jnp.float32) for item_w in (gain_attn, w_query, b_query, key_weight, key_bias, value_weight, value_bias, w_output, gain_mlp, w_gate, w_up, w_down)))
    sequences = inputs.astype(jnp.float32).reshape(N_DP, SEQ, MODEL_WIDTH)
    checked_layer = jax.checkpoint(layer)

    def run(all_seqs, *params):
        return lax.map(lambda one_seq: checked_layer(one_seq, *params), all_seqs)
    result, pullback = jax.vjp(run, sequences, *weights)
    grads = pullback(cotangent.astype(jnp.float32).reshape(N_DP, SEQ, MODEL_WIDTH))
    return (result.reshape(TOKENS, MODEL_WIDTH).astype(jnp.bfloat16), grads[0].reshape(TOKENS, MODEL_WIDTH).astype(jnp.bfloat16), grads[1], grads[2], grads[3], grads[4], grads[5], grads[6], grads[7], grads[8], grads[9], grads[10], grads[11], grads[12])
```

```python
import math

import jax
import jax.numpy as jnp
from jax import lax
from jax.sharding import Mesh, PartitionSpec as P

HEAD = 128
EPS = 1e-06
ROPE_BASE = 1000000.0
F32 = jnp.float32
BF16 = jnp.bfloat16


def rope(rows, positions, direction):
    half = HEAD // 2
    n = rows.shape[0]
    heads = rows.shape[1] // HEAD
    freqs = ROPE_BASE ** (-(jnp.arange(half, dtype=F32) * 2.0 / HEAD))
    angles = positions.astype(F32)[:, None] * freqs[None, :]
    cosine = jnp.cos(angles)[:, None, :]
    sine = direction * jnp.sin(angles)[:, None, :]
    shaped = rows.reshape(n, heads, HEAD)
    a = shaped[..., :half]
    b = shaped[..., half:]
    turned = jnp.concatenate([a * cosine - b * sine, b * cosine + a * sine], -1)
    return turned.reshape(n, heads * HEAD)


def nn(a, b):
    return lax.dot_general(a, b, (((1,), (0,)), ((), ())), preferred_element_type=F32)


def nt(a, b):
    return lax.dot_general(a, b, (((1,), (1,)), ((), ())), preferred_element_type=F32)


def tn(a, b):
    return lax.dot_general(a, b, (((0,), (0,)), ((), ())), preferred_element_type=F32)


def shards(x, g1, wq, bq, wk, bk, wv, bv, wo, g2, wg, wu, wd, cot):
    pods, D, R, C = (lax.axis_size(a) for a in ("pod", "dp", "row", "col"))
    width = x.shape[1] * C
    rows_f = g1.shape[0]
    tok = x.shape[0] // C
    qw, kw = wq.shape[1], wk.shape[1]
    heads, kv = qw // HEAD, kw // HEAD
    units_r = wg.shape[1]
    both = jnp.concatenate([x, cot], 1).reshape(C, tok, 2 * x.shape[1])
    both = lax.all_to_all(both, "col", 0, 0, tiled=True).reshape(C, tok, 2, x.shape[1])
    both = both.transpose(2, 1, 0, 3).reshape(2, tok, width)
    x_own, cot_own = both[0], both[1]
    x_pair = lax.all_gather(x_own, "row", axis=0, tiled=True)
    bias = jnp.concatenate([bq, bk, bv])
    nb = -(-bias.shape[0] // rows_f)
    bias_cols = jnp.pad(bias, (0, nb * rows_f - bias.shape[0])).reshape(nb, rows_f).T
    pack = jnp.concatenate([wq, wk, wv, g1[:, None], g2[:, None], bias_cols], 1)
    pack = lax.all_gather(pack, ("col", "pod", "dp"), axis=0, tiled=True)
    ow = qw + 2 * kw
    w_in = pack[:, :ow]
    gain1 = pack[:, ow].astype(F32)
    gain2 = pack[:, ow + 1].astype(F32)
    b_all = pack[: width // C, ow + 2 :].reshape(pods * D, rows_f, nb).transpose(0, 2, 1)
    b_all = b_all.reshape(pods * D, nb * rows_f)
    lq, lk = bq.shape[0], bk.shape[0]
    bias_in = jnp.concatenate(
        [
            b_all[:, :lq].reshape(-1),
            b_all[:, lq : lq + lk].reshape(-1),
            b_all[:, lq + lk : lq + 2 * lk].reshape(-1),
        ]
    ).astype(F32)
    w_out = lax.all_gather(wo, ("pod", "dp", "col"), axis=0)
    w_out = w_out.reshape(pods * D, C, wo.shape[0], wo.shape[1]).transpose(0, 2, 1, 3)
    w_out = w_out.reshape(qw, width)
    if pods > 1:
        wg, wu, wd = (lax.all_gather(w, "pod", axis=0) for w in (wg, wu, wd))
    else:
        wg, wu, wd = wg[None], wu[None], wd[None]
    share = units_r // (D * C)

    def spread(w):
        u = units_r // (pods * D)
        w = w.reshape(pods, rows_f, pods, D, u).transpose(3, 2, 4, 0, 1).reshape(D, C, share, pods, rows_f)
        return w.transpose(1, 0, 3, 4, 2)

    gu = jnp.concatenate([spread(wg), spread(wu)], -1)
    gu = gu.reshape(C * D, pods, rows_f, 2 * share)
    gu = lax.all_to_all(gu, ("col", "dp"), 0, 0, tiled=True)
    gu = gu.reshape(C, D, pods, rows_f, 2 * share).transpose(0, 2, 1, 3, 4).reshape(width, 2 * share)
    gu = lax.all_gather(gu, "row", axis=0)
    w_g = jnp.concatenate([gu[i, :, :share] for i in range(R)], 1)
    w_u = jnp.concatenate([gu[i, :, share:] for i in range(R)], 1)
    dn = wd.reshape(C, share, wd.shape[2])
    dn = lax.all_to_all(dn, "col", 0, 0, tiled=True).transpose(1, 0, 2).reshape(share, width)
    w_d = lax.all_gather(dn, "row", axis=0, tiled=True)
    cot_all = lax.all_gather(cot_own, ("dp", "col"), axis=0, tiled=True)
    c = lax.axis_index("col")
    sub = jnp.arange(tok, dtype=jnp.int32)
    positions = (jnp.arange(R, dtype=jnp.int32)[:, None] * (tok * C) + c * tok + sub[None, :]).reshape(-1)
    key_pos = (
        jnp.arange(C, dtype=jnp.int32)[:, None, None] * tok
        + jnp.arange(R, dtype=jnp.int32)[None, :, None] * (tok * C)
        + sub[None, None, :]
    ).reshape(-1)
    xp = x_pair.astype(F32)
    inv1 = lax.rsqrt(jnp.mean(xp * xp, 1, keepdims=True) + EPS)
    normed1 = (xp * inv1 * gain1).astype(BF16)
    proj = nn(normed1, w_in) + bias_in
    q = rope(proj[:, :qw], positions, 1.0).astype(BF16)
    k = rope(proj[:, qw : qw + kw], positions, 1.0).astype(BF16)
    v = proj[:, qw + kw :].astype(BF16)
    kv_all = lax.all_gather(jnp.concatenate([k, v], 1), "col", axis=0, tiled=True)
    ka, va = kv_all[:, :kw], kv_all[:, kw:]
    nq = q.shape[0]
    ns = ka.shape[0]
    group = heads // kv
    q4 = q.reshape(nq, kv, group, HEAD)
    k3 = ka.reshape(ns, kv, HEAD)
    v3 = va.reshape(ns, kv, HEAD)
    scores = jnp.einsum("ikgd,jkd->kgij", q4, k3, preferred_element_type=F32) * HEAD ** (-0.5)
    admitted = key_pos[None, :] <= positions[:, None]
    scores = jnp.where(admitted, scores, -1e30)
    top = jnp.max(scores, -1, keepdims=True)
    expo = jnp.exp(scores - top)
    total = jnp.sum(expo, -1, keepdims=True)
    probs = expo / total
    probs_low = probs.astype(BF16)
    att = jnp.einsum("kgij,jkd->ikgd", probs_low, v3, preferred_element_type=F32)
    att = att.reshape(nq, qw).astype(BF16)
    part = nn(att, w_out).astype(BF16)
    mid = x_own.astype(F32) + lax.psum_scatter(part, "row", scatter_dimension=0, tiled=True).astype(F32)
    inv2 = lax.rsqrt(jnp.mean(mid * mid, 1, keepdims=True) + EPS)
    normed2 = (mid * inv2 * gain2).astype(BF16)
    n2 = lax.all_gather(normed2, ("dp", "col"), axis=0, tiled=True)
    gate = nn(n2, w_g)
    up = nn(n2, w_u)
    d_hidden = nt(cot_all, w_d)
    sig = jax.nn.sigmoid(gate)
    silu = gate * sig
    hidden = (silu * up).astype(BF16)
    d_gate = (d_hidden * up * sig * (1.0 + gate * (1.0 - sig))).astype(BF16)
    d_up = (d_hidden * silu).astype(BF16)
    d_n2 = (nt(d_gate, w_g) + nt(d_up, w_u)).astype(BF16)
    d_n2 = lax.psum_scatter(d_n2, ("dp", "col"), scatter_dimension=0, tiled=True).astype(F32)
    out_part = nn(hidden, w_d).astype(BF16)
    out_sum = lax.psum_scatter(out_part, ("dp", "col"), scatter_dimension=0, tiled=True)
    outputs = (mid + out_sum.astype(F32)).astype(BF16)
    g_down = tn(hidden, cot_all).astype(BF16)
    g_gate = tn(n2, d_gate).astype(BF16)
    g_up = tn(n2, d_up).astype(BF16)
    g_gu = jnp.stack(
        [
            jnp.concatenate([g_gate[:, i * share : (i + 1) * share], g_up[:, i * share : (i + 1) * share]], 1)
            for i in range(R)
        ]
    )
    g_gu = lax.psum_scatter(g_gu, "row", scatter_dimension=0, tiled=False)
    g_gu = g_gu.reshape(C, pods, D, rows_f, 2 * share).transpose(0, 2, 1, 3, 4).reshape(C * D, pods, rows_f, 2 * share)
    g_gu = lax.all_to_all(g_gu, ("col", "dp"), 0, 0, tiled=True).reshape(C, D, pods, rows_f, 2, share)
    g_dn = lax.psum_scatter(g_down, "row", scatter_dimension=0, tiled=True)
    g_dn = g_dn.reshape(share, C, wd.shape[2]).transpose(1, 0, 2)
    g_dn = lax.all_to_all(g_dn, "col", 0, 0, tiled=True)
    u = units_r // (pods * D)
    g_dn = g_dn.reshape(pods, u, wd.shape[2])

    def unspread(g):
        g = g.transpose(1, 0, 4, 2, 3).reshape(D, pods, u, pods, rows_f)
        return g.transpose(3, 4, 1, 0, 2).reshape(pods, rows_f, units_r)

    gg, gu_ = unspread(g_gu[..., 0, :]), unspread(g_gu[..., 1, :])
    if pods > 1:
        gg, gu_, g_dn = (lax.psum_scatter(t, "pod", scatter_dimension=0, tiled=False) for t in (gg, gu_, g_dn))
    else:
        gg, gu_, g_dn = gg[0], gu_[0], g_dn[0]
    weighted = d_n2 * gain2
    inner = jnp.sum(weighted * mid, 1, keepdims=True)
    cot_f = cot_own.astype(F32)
    d_mid = cot_f + inv2 * weighted - mid * (inv2 * inv2 * inv2) * inner / width
    gain_term2 = jnp.sum(d_n2 * mid * inv2, 0)
    dm_pair = lax.all_gather(d_mid.astype(BF16), "row", axis=0, tiled=True)
    g_wo = tn(att, dm_pair).astype(BF16)
    g_wo = g_wo.reshape(pods * D, wo.shape[0], C, wo.shape[1]).transpose(0, 2, 1, 3)
    g_wo = lax.psum_scatter(
        g_wo.reshape(pods * D * C, wo.shape[0], wo.shape[1]), ("pod", "dp", "col"), scatter_dimension=0, tiled=False
    )
    d_att = nt(dm_pair, w_out).astype(BF16)
    da4 = d_att.reshape(q4.shape)
    d_probs = jnp.einsum("ikgd,jkd->kgij", da4, v3, preferred_element_type=F32)
    centre = jnp.sum(probs * d_probs, -1, keepdims=True)
    d_scores = (probs * (d_probs - centre)).astype(BF16)
    scale = HEAD ** (-0.5)
    d_q = jnp.einsum("kgij,jkd->ikgd", d_scores, k3, preferred_element_type=F32).reshape(nq, qw) * scale
    d_k = jnp.einsum("kgij,ikgd->jkd", d_scores, q4, preferred_element_type=F32).reshape(ns, kw) * scale
    d_v = jnp.einsum("kgij,ikgd->jkd", probs_low, da4, preferred_element_type=F32).reshape(ns, kw)
    dkv = jnp.concatenate([d_k, d_v], 1).astype(BF16)
    dkv = lax.psum_scatter(dkv, "col", scatter_dimension=0, tiled=True).astype(F32)
    d_in = jnp.concatenate(
        [rope(d_q, positions, -1.0), rope(dkv[:, :kw], positions, -1.0), dkv[:, kw:]], 1
    )
    d_in_low = d_in.astype(BF16)
    d_n1 = nt(d_in_low, w_in).astype(BF16)
    d_n1 = lax.psum_scatter(d_n1, "row", scatter_dimension=0, tiled=True).astype(F32)
    xf = x_own.astype(F32)
    inv_own = lax.rsqrt(jnp.mean(xf * xf, 1, keepdims=True) + EPS)
    weighted1 = d_n1 * gain1
    inner1 = jnp.sum(weighted1 * xf, 1, keepdims=True)
    grad_x = (d_mid + inv_own * weighted1 - xf * (inv_own * inv_own * inv_own) * inner1 / width).astype(BF16)
    gain_term1 = jnp.sum(d_n1 * xf * inv_own, 0)
    g_in = tn(normed1, d_in_low).astype(BF16)
    gb = jnp.sum(d_in_low.astype(F32), 0).astype(BF16)
    gb_parts = jnp.concatenate(
        [
            gb[:qw].reshape(pods * D, lq),
            gb[qw : qw + kw].reshape(pods * D, lk),
            gb[qw + kw :].reshape(pods * D, lk),
            jnp.zeros((pods * D, nb * rows_f - bias.shape[0]), BF16),
        ],
        1,
    )
    gb_cols = gb_parts.reshape(1, pods * D, nb, rows_f).transpose(0, 1, 3, 2)
    gb_cols = jnp.broadcast_to(gb_cols, (C, pods * D, rows_f, nb)).reshape(width, nb)
    g_pack = jnp.concatenate(
        [g_in, gain_term1.astype(BF16)[:, None], gain_term2.astype(BF16)[:, None], gb_cols], 1
    )
    g_pack = lax.psum_scatter(g_pack, ("col", "pod", "dp"), scatter_dimension=0, tiled=True).astype(F32)
    gains = lax.psum(g_pack[:, ow : ow + 2], "row")
    g_bias = g_pack[:, ow + 2 :].T.reshape(-1)
    fin = jnp.concatenate([outputs.reshape(tok, C, -1), grad_x.reshape(tok, C, -1)], 2).transpose(1, 0, 2)
    fin = lax.all_to_all(fin, "col", 0, 0, tiled=True).reshape(C * tok, -1)
    fw = x.shape[1]
    return (
        fin[:, :fw],
        fin[:, fw:],
        gains[:, 0],
        g_pack[:, :qw],
        g_bias[:lq],
        g_pack[:, qw : qw + kw],
        g_bias[lq : lq + lk],
        g_pack[:, qw + kw : ow],
        g_bias[lq + lk : lq + 2 * lk],
        g_wo.astype(F32),
        gains[:, 1],
        gg.astype(F32),
        gu_.astype(F32),
        g_dn.astype(F32),
    )


def solution(mesh):
    team = math.gcd(mesh.shape["dp"], 4)
    names = {"dp": ("pod", "dp"), "row": ("row",), "col": ("col",)}
    sizes = (mesh.shape["dp"] // team, team, mesh.shape["row"], mesh.shape["col"])
    grid = Mesh(mesh.devices.reshape(sizes), ("pod", "dp", "row", "col"))

    def spec(*dims):
        return P(*(tuple(n for a in d for n in names[a]) for d in dims))

    act = spec(("dp", "row"), ("col",))
    vec_f = spec(("col", "dp"))
    w_in = spec(("col", "dp"), ("row",))
    vec_r = spec(("row", "dp"))
    w_out = spec(("row", "dp"), ("col",))
    return jax.shard_map(
        shards,
        mesh=grid,
        in_specs=(act, vec_f, w_in, vec_r, w_in, vec_r, w_in, vec_r, w_out, vec_f, w_in, w_in, w_out, act),
        out_specs=(act, act, vec_f, w_in, vec_r, w_in, vec_r, w_in, vec_r, w_out, vec_f, w_in, w_in, w_out),
        check_vma=False,
    )
```
